32 devices in a mesh: sub: 2 (over x), row: 16 (over z, y, core).
Axes of the slice: x: 2, y: 2, z: 4, core: 2. Of those that a mesh axis runs over, the one named last changes fastest.
Arguments:
- diag_blocks: float32 [512, 128, 128], P(('sub', 'row')), parts along dimension 0, may hold values from -0.05 to 16, as said below
- coupling: float32 [512, 3, 128, 128], P(('sub', 'row')), parts along dimension 0, may hold values from -0.05 to 0.05
- offsets: int32 [512, 3], P(('sub', 'row')), parts along dimension 0, may hold values from 1 to 4, as said below
- mass: float32 [65536], P(('sub', 'row')), parts along dimension 0, may hold values from 0.5 to 2
- initial_modes: float32 [32, 65536], P(None, ('sub', 'row')), parts along dimension 1, may hold values from -6 to 6
Outputs:
- mass_density: float32 [65536], P(('sub', 'row')), parts along dimension 0
- energy_density: float32 [65536], P(('sub', 'row')), parts along dimension 0
The draws below stay inside these ranges and needn't reach their ends.
There are 2 independent parts, one for each index of `sub`. The reference program is written for one: setup_inputs(seed, part) draws one part's arguments, and reference() takes and returns one part's arrays. A program takes and returns all parts, laid end to end along the dimension named above; each array names one. Nothing has to cross between parts.
Inputs may be any that keep to these rules, and one draw needn't show every extreme that they name: `diag_blocks`: each block is symmetric; entries off a block's diagonal lie in -0.05 to 0.05, its diagonal entries in 1 to 16. The 3 offsets of a block row are distinct.
All inputs are finite; a program needn't handle non-finite values.
Results may differ from the reference program's by a relative error of at most 0.0003.
Values sent between devices are 32-bit elements; how exact they have to be, the bound alone decides.
A program may use at most 128 MiB of HBM per device.

```python
import math
import jax
import jax.numpy as jnp
from jax import lax

BLK = 128
MODES = 32
SLOTS = 3
REACH = 4
ITERS = 3
PURIFY = 28
NBLK = 256
N = 32768


def draw_diag_blocks(key, part):
    key_off, key_diag = jax.random.split(key)
    shape = (NBLK, BLK, BLK)
    couplings = jax.random.uniform(key_off, shape, jnp.float32, -0.05, 0.05)
    diagonal = jnp.exp(jax.random.uniform(key_diag, (NBLK, BLK), jnp.float32, 0.0, jnp.log(10.0)))
    identity = jnp.eye(BLK, dtype=jnp.float32)
    symmetric = 0.5 * (couplings + jnp.swapaxes(couplings, 1, 2))
    return symmetric * (1.0 - identity)[None, :, :] + identity[None, :, :] * diagonal[:, :, None]


def draw_offsets(key, part):
    scores = jax.random.randint(key, (NBLK, REACH), 0, 1 << 20) * REACH + jnp.arange(REACH, dtype=jnp.int32)[None, :]
    ranking = jnp.argsort(scores, axis=1)
    return (ranking[:, :SLOTS] + 1).astype(jnp.int32)


def steps_of(key, extent, cuts, smallest, largest):
    gain, own = 1.0, jax.random.fold_in(key, 6)
    for axis_at, blocks in cuts:
        steps = jnp.exp(jax.random.uniform(jax.random.fold_in(own, axis_at), (blocks,), jnp.float32, smallest / len(cuts), largest / len(cuts)))
        gain = gain * jnp.repeat(steps, extent[axis_at] // blocks).reshape([-1 if axis == axis_at else 1 for axis in range(len(extent))])
    return gain


def gaussian(own_key, dims, deviation, limit, pieces=(), held_as=jnp.bfloat16):
    entries = jax.random.normal(own_key, dims, jnp.float32) * deviation
    if len(pieces) > 0:
        entries = steps_of(own_key, dims, pieces, -0.22, 0.18) * entries
    return jnp.clip(entries, min=-limit, max=limit).astype(held_as)


def setup_inputs(seed: int = 0, part: int = 0) -> dict:
    arg_keys = jax.random.split(jax.random.key(seed), 6)
    part_splits = jax.random.split(jax.random.fold_in(arg_keys[5], part), 6)
    diag_blocks = draw_diag_blocks(jax.random.fold_in(jax.random.fold_in(arg_keys[5], part), 71), part)
    coupling = jnp.clip(jax.random.uniform(part_splits[1], (NBLK, SLOTS, BLK, BLK), jnp.float32, -0.05, 0.05) * steps_of(part_splits[1], (NBLK, SLOTS, BLK, BLK), ((0, 16),), -0.4, 0.0), -0.05, 0.05)
    offsets = draw_offsets(jax.random.fold_in(jax.random.fold_in(arg_keys[5], part), 71), part)
    mass = jnp.clip(jnp.exp(math.log(2.0) - 1.3862944 * jax.random.uniform(part_splits[3], (N,), jnp.float32) ** steps_of(part_splits[3], (N,), ((0, 16),), -0.2, 0.2)), 0.5, 2.0)
    initial_modes = gaussian(part_splits[4], (MODES, N), 1.0, 6.0, ((1, 16),), jnp.float32)
    return {"diag_blocks": diag_blocks, "coupling": coupling, "offsets": offsets, "mass": mass, "initial_modes": initial_modes}


PRECISE = lax.Precision.HIGHEST

def stiffness_apply(vectors, diag_blocks, coupling, offsets):
    rowcount = vectors.shape[0]
    block_count = diag_blocks.shape[0]
    block_width = diag_blocks.shape[1]
    blocked = vectors.reshape(rowcount, block_count, block_width)
    result = jnp.einsum('nbk,bkj->nbj', blocked, diag_blocks, precision=PRECISE)
    targets = jnp.arange(block_count, dtype=jnp.int32)[:, None] - offsets
    present = (targets >= 0).astype(vectors.dtype)
    clipped = jnp.maximum(targets, 0).astype(jnp.int32)
    gathered = blocked[:, clipped, :] * present[None, :, :, None]
    result = result + jnp.einsum('nbsk,bsjk->nbj', gathered, coupling, precision=PRECISE)
    products = jnp.einsum('nbk,bskj->nbsj', blocked, coupling, precision=PRECISE) * present[None, :, :, None]
    result = result.at[:, clipped, :].add(products)
    return result.reshape(rowcount, block_count * block_width)

def purify(matrix, occupied, steps_count):
    order = matrix.shape[0]
    identity = jnp.eye(order, dtype=matrix.dtype)
    diagonal = jnp.diagonal(matrix)
    center = jnp.sum(diagonal) / order
    radius = lax.optimization_barrier(jnp.sum(jnp.abs(matrix), axis=1)) - jnp.abs(diagonal)
    highest = jnp.max(diagonal + radius)
    lowest = jnp.min(diagonal - radius)
    factor = jnp.minimum(occupied / jnp.maximum(highest - center, 1e-06), (order - occupied) / jnp.maximum(center - lowest, 1e-06))
    initial = factor / order * (center * identity - matrix) + occupied / order * identity

    def purify_step(index, density):
        square = jnp.dot(density, density, precision=PRECISE)
        cube = jnp.dot(square, density, precision=PRECISE)
        numerator = jnp.trace(square - cube)
        denominator = jnp.trace(density - square)
        safe_denominator = jnp.where(jnp.abs(denominator) > 1e-12, denominator, 1.0)
        ratio = jnp.clip(numerator / safe_denominator, 0.0, 1.0)
        upward = ((1.0 + ratio) * square - cube) / jnp.maximum(ratio, 0.5)
        downward = ((1.0 - 2.0 * ratio) * density + (1.0 + ratio) * square - cube) / jnp.maximum(1.0 - ratio, 0.5)
        return jnp.where(ratio >= 0.5, upward, downward)
    return lax.fori_loop(0, steps_count, purify_step, initial)

def ritz_basis(gram_stiff, gram_mass, modes_wanted, steps_count):
    order = gram_stiff.shape[0]
    gram_stiff = 0.5 * (gram_stiff + gram_stiff.T)
    gram_mass = 0.5 * (gram_mass + gram_mass.T)
    scaling = lax.rsqrt(jnp.diagonal(gram_mass) + 1e-06)
    stiff_scaled = scaling[:, None] * gram_stiff * scaling[None, :]
    mass_scaled = scaling[:, None] * gram_mass * scaling[None, :]
    factor_low = jnp.linalg.cholesky(mass_scaled)
    identity = jnp.eye(order, dtype=gram_stiff.dtype)
    inverse_low = lax.linalg.triangular_solve(factor_low, identity, left_side=True, lower=True)
    reduced = jnp.dot(jnp.dot(inverse_low, stiff_scaled, precision=PRECISE), inverse_low.T, precision=PRECISE)
    reduced = 0.5 * (reduced + reduced.T)
    if order > modes_wanted:
        projector = purify(reduced, modes_wanted, steps_count)
        columns = projector[:, :modes_wanted]
    else:
        columns = identity
    correlation = jnp.dot(columns.T, columns, precision=PRECISE)
    correlation_low = jnp.linalg.cholesky(correlation)
    orthonormal = lax.linalg.triangular_solve(correlation_low, columns.T, left_side=True, lower=True).T
    coefficients = scaling[:, None] * jnp.dot(inverse_low.T, orthonormal, precision=PRECISE)
    projected = jnp.dot(jnp.dot(orthonormal.T, reduced, precision=PRECISE), orthonormal, precision=PRECISE)
    return (coefficients, 0.5 * (projected + projected.T))

def reference(diag_blocks, coupling, offsets, mass, initial_modes):
    stiff_diag = jnp.diagonal(diag_blocks, axis1=1, axis2=2).reshape(-1)

    def gram_pair(basis, stiff_basis):
        gram_stiff = jnp.dot(basis, stiff_basis.T, precision=PRECISE)
        gram_mass = jnp.dot(basis * mass[None, :], basis.T, precision=PRECISE)
        return (gram_stiff, gram_mass)
    stiff_initial = stiffness_apply(initial_modes, diag_blocks, coupling, offsets)
    gram_stiff, gram_mass = gram_pair(initial_modes, stiff_initial)
    coefficients, projected = ritz_basis(gram_stiff, gram_mass, MODES, PURIFY)
    modes_now = jnp.dot(coefficients.T, initial_modes, precision=PRECISE)
    stiff_modes = jnp.dot(coefficients.T, stiff_initial, precision=PRECISE)
    directions = None
    stiff_directions = None
    for iteration in range(ITERS):
        residual = stiff_modes - jnp.dot(projected, modes_now * mass[None, :], precision=PRECISE)
        precond = residual / stiff_diag[None, :]
        stiff_precond = stiffness_apply(precond, diag_blocks, coupling, offsets)
        if directions is None:
            basis = jnp.concatenate([modes_now, precond], axis=0)
            stiff_basis = jnp.concatenate([stiff_modes, stiff_precond], axis=0)
        else:
            basis = jnp.concatenate([modes_now, precond, directions], axis=0)
            stiff_basis = jnp.concatenate([stiff_modes, stiff_precond, stiff_directions], axis=0)
        gram_stiff, gram_mass = gram_pair(basis, stiff_basis)
        coefficients, projected = ritz_basis(gram_stiff, gram_mass, MODES, PURIFY)
        directions = jnp.dot(coefficients[MODES:].T, basis[MODES:], precision=PRECISE)
        stiff_directions = jnp.dot(coefficients[MODES:].T, stiff_basis[MODES:], precision=PRECISE)
        modes_now = jnp.dot(coefficients.T, basis, precision=PRECISE)
        stiff_modes = jnp.dot(coefficients.T, stiff_basis, precision=PRECISE)
    weight = modes_now.shape[1] / MODES
    mass_density = weight * mass * lax.optimization_barrier(jnp.sum(modes_now * modes_now, axis=0))
    energy_density = weight * lax.optimization_barrier(jnp.sum(modes_now * stiff_modes, axis=0))
    return (mass_density, energy_density)
```

```python
import functools

import jax
import jax.numpy as jnp
from jax import lax
from jax.experimental import pallas as pl
from jax.experimental.pallas import tpu as pltpu
from jax.sharding import PartitionSpec as P

MODES = 32
REACH = 4
ITERS = 3
PURIFY = 28
LANES = 128
TILE = 8


PRECISE = lax.Precision.HIGHEST
MESH = pl.DeviceIdType.MESH
NT = (((1,), (1,)), ((), ()))
NN = (((1,), (0,)), ((), ()))


def dot(a, b, dims=NN):
    return lax.dot_general(a, b, dims, precision=PRECISE, preferred_element_type=jnp.float32)


def split(a):
    high = a.astype(jnp.bfloat16)
    return high, (a - high.astype(jnp.float32)).astype(jnp.bfloat16)


def dot3(a, b, dims=NN):
    (ah, al), (bh, bl) = a, b
    term = functools.partial(lax.dot_general, dimension_numbers=dims, preferred_element_type=jnp.float32)
    return term(ah, bh) + (term(ah, bl) + term(al, bh))


def gram_kernel(ring, order, s_ref, ks_ref, m_ref, out_ref, part, recv, done, send1, recv1, send2, recv2):
    tiles = order // TILE
    me = lax.axis_index("row")
    barrier = pltpu.get_barrier_semaphore()

    @pl.loop(1, ring)
    def _(step):
        peer = lax.rem(me + step, ring)
        pl.semaphore_signal(barrier, inc=1, device_id={"row": peer}, device_id_type=MESH)

    basis = s_ref[...]
    stiff = dot(basis[:order], ks_ref[...], NT)
    massed = dot(basis[:order] * m_ref[...], basis, NT)
    r = lax.broadcasted_iota(jnp.int32, (order, LANES), 0)
    c = lax.broadcasted_iota(jnp.int32, (order, LANES), 1)
    diagonal = jnp.sum(jnp.where(r == c, massed, 0.0), axis=1, keepdims=True)
    packed = jnp.where(c < order, jnp.where(r <= c, stiff, massed), jnp.where(c == order, diagonal, 0.0))
    for t in range(tiles):
        part[t] = packed[t * TILE : (t + 1) * TILE]
    pl.semaphore_wait(barrier, ring - 1)

    def scatter(t):
        return pltpu.make_async_remote_copy(
            src_ref=part.at[t], dst_ref=recv.at[me], send_sem=send1.at[t], recv_sem=recv1.at[me],
            device_id={"row": t}, device_id_type=MESH)

    def arrival(source):
        return pltpu.make_async_remote_copy(
            src_ref=part.at[0], dst_ref=recv.at[source], send_sem=send1.at[0], recv_sem=recv1.at[source],
            device_id={"row": source}, device_id_type=MESH)

    def spread(peer):
        return pltpu.make_async_remote_copy(
            src_ref=done.at[me], dst_ref=done.at[me], send_sem=send2.at[peer], recv_sem=recv2.at[me],
            device_id={"row": peer}, device_id_type=MESH)

    def gathered(t):
        return pltpu.make_async_remote_copy(
            src_ref=done.at[t], dst_ref=done.at[t], send_sem=send2.at[0], recv_sem=recv2.at[t],
            device_id={"row": t}, device_id_type=MESH)

    @pl.loop(0, tiles)
    def _(t):
        @pl.when(t != me)
        def _():
            scatter(t).start()

    @pl.when(me < tiles)
    def _():
        recv[me] = part[me]

        @pl.loop(0, ring)
        def _(source):
            @pl.when(source != me)
            def _():
                arrival(source).wait_recv()

        done[me] = jnp.sum(recv[...], axis=0)

        @pl.loop(1, ring)
        def _(step):
            spread(lax.rem(me + step, ring)).start()

    @pl.loop(0, tiles)
    def _(t):
        @pl.when(t != me)
        def _():
            gathered(t).wait_recv()

    for t in range(tiles):
        out_ref[t * TILE : (t + 1) * TILE] = done[t]

    @pl.loop(0, tiles)
    def _(t):
        @pl.when(t != me)
        def _():
            scatter(t).wait_send()

    @pl.when(me < tiles)
    def _():
        @pl.loop(1, ring)
        def _(step):
            spread(lax.rem(me + step, ring)).wait_send()


def gram_pair(basis, stiff_basis, mass, order):
    ring = lax.axis_size("row")
    tiles = order // TILE
    assert tiles <= ring
    vmem = pl.BlockSpec(memory_space=pltpu.VMEM)
    return pl.pallas_call(
        functools.partial(gram_kernel, ring, order),
        out_shape=jax.ShapeDtypeStruct((order, LANES), jnp.float32),
        in_specs=[vmem] * 3,
        out_specs=vmem,
        scratch_shapes=[
            pltpu.VMEM((tiles, TILE, LANES), jnp.float32),
            pltpu.VMEM((ring, TILE, LANES), jnp.float32),
            pltpu.VMEM((tiles, TILE, LANES), jnp.float32),
            pltpu.SemaphoreType.DMA((tiles,)),
            pltpu.SemaphoreType.DMA((ring,)),
            pltpu.SemaphoreType.DMA((ring,)),
            pltpu.SemaphoreType.DMA((tiles,)),
        ],
        compiler_params=pltpu.CompilerParams(collective_id=order // MODES, has_side_effects=True),
        name=f"gram{order}",
    )(basis, stiff_basis, mass)


def eliminate(rows, other, start):
    r = lax.broadcasted_iota(jnp.int32, (MODES, 1), 0)
    scale = jnp.zeros((MODES, 1), jnp.float32)
    for j in range(MODES):
        column = rows[:, start + j : start + j + 1]
        pivot = rows[j : j + 1, start + j : start + j + 1]
        factor = jnp.where(r > j, column * (1.0 / pivot), 0.0)
        scale = jnp.where(r == j, lax.rsqrt(pivot), scale)
        top, top_other = rows[j : j + 1], other[j : j + 1]
        rows = rows - factor * top
        other = other - factor * top_other
    return rows * scale, other * scale


def ritz_kernel(order, steps_count, m_ref, coef_ref, h_ref):
    shape = (LANES, LANES)
    r = lax.broadcasted_iota(jnp.int32, shape, 0)
    c = lax.broadcasted_iota(jnp.int32, shape, 1)
    eye = (r == c) & (r < order)
    identity = jnp.where(eye, 1.0, 0.0)
    inside = (r < order) & (c < order)
    packed = m_ref[...]
    if order < LANES:
        packed = jnp.concatenate([packed, jnp.zeros((LANES - order, LANES), jnp.float32)], axis=0)
    flipped = packed.T
    g_col = lax.rsqrt(packed[:, order : order + 1] + 1e-06)
    g_row = lax.rsqrt(flipped[order : order + 1, :] + 1e-06)
    stiff = jnp.where(inside, jnp.where(r <= c, packed, flipped), 0.0)
    massed = jnp.where(inside, jnp.where(r > c, packed, flipped), 0.0)
    massed = jnp.where(eye, packed[:, order : order + 1], massed)
    stiff = g_col * stiff * g_row
    massed = g_col * massed * g_row
    bands = []
    below = identity
    for start in range(0, order, MODES):
        rows, other = eliminate(massed[start : start + MODES], below[start : start + MODES], start)
        bands.append(other)
        if start + MODES < order:
            across = rows.T
            massed = jnp.where(r >= start + MODES, massed - dot(across, rows), massed)
            below = jnp.where(r >= start + MODES, below - dot(across, other), below)
    if order < LANES:
        bands.append(jnp.zeros((LANES - order, LANES), jnp.float32))
    inverse = jnp.concatenate(bands, axis=0)
    reduced = dot(dot(inverse, stiff), inverse, NT)
    reduced = 0.5 * (reduced + reduced.T)
    if order > MODES:
        diagonal = jnp.sum(jnp.where(eye, reduced, 0.0), axis=1, keepdims=True)
        real = lax.broadcasted_iota(jnp.int32, (LANES, 1), 0) < order
        center = jnp.sum(diagonal, axis=(0, 1), keepdims=True) / order
        radius = jnp.sum(jnp.abs(reduced), axis=1, keepdims=True) - jnp.abs(diagonal)
        highest = jnp.max(jnp.where(real, diagonal + radius, -jnp.inf), axis=(0, 1), keepdims=True)
        lowest = jnp.min(jnp.where(real, diagonal - radius, jnp.inf), axis=(0, 1), keepdims=True)
        factor = jnp.minimum(
            MODES / jnp.maximum(highest - center, 1e-06),
            (order - MODES) / jnp.maximum(center - lowest, 1e-06),
        )
        initial = factor / order * (center * identity - reduced) + MODES / order * identity

        def purify_step(index, density):
            halves = split(density)
            square = dot3(halves, halves)
            cube = dot3(split(square), halves)
            numerator = jnp.sum(square * (identity - density), axis=(0, 1), keepdims=True)
            denominator = jnp.sum(jnp.where(eye, density - square, 0.0), axis=(0, 1), keepdims=True)
            safe = jnp.where(jnp.abs(denominator) > 1e-12, denominator, 1.0)
            ratio = jnp.clip(numerator / safe, 0.0, 1.0)
            up = ratio >= 0.5
            share = 1.0 / jnp.where(up, ratio, 1.0 - ratio)
            keep = jnp.where(up, 0.0, (1.0 - 2.0 * ratio) * share)
            return keep * density + share * ((1.0 + ratio) * square - cube)

        projector = lax.fori_loop(0, steps_count, purify_step, initial)
        columns = projector.T[:MODES]
        correlation = dot(columns, columns, NT)
        _, orthonormal = eliminate(correlation, columns, 0)
    else:
        orthonormal = identity[:MODES]
    coef_ref[...] = dot(orthonormal, inverse) * g_row
    half = dot(orthonormal, reduced)
    h_ref[...] = 0.5 * (dot(half, orthonormal, NT) + dot(orthonormal, half, NT))


def ritz_basis(packed, order):
    vmem = pl.BlockSpec(memory_space=pltpu.VMEM)
    return pl.pallas_call(
        functools.partial(ritz_kernel, order, PURIFY),
        out_shape=(
            jax.ShapeDtypeStruct((MODES, LANES), jnp.float32),
            jax.ShapeDtypeStruct((MODES, MODES), jnp.float32),
        ),
        in_specs=[vmem],
        out_specs=(vmem, vmem),
        name=f"ritz{order}",
    )(packed)


def from_behind(value, axis, steps):
    count = lax.axis_size(axis)
    initial, last = (max(0, -steps), min(count, count - steps))
    return lax.ppermute(value, axis, [(source, source + steps) for source in range(initial, last)])


def one_hot_table(positions, extent):
    return (positions[..., None] == jnp.arange(extent, dtype=jnp.int32)).astype(jnp.float32)


def stiffness_apply(vectors, diag_blocks, coupling, offsets):
    rowcount = vectors.shape[0]
    block_count = diag_blocks.shape[0]
    block_width = diag_blocks.shape[1]
    blocked = vectors.reshape(rowcount, block_count, block_width)
    result = jnp.einsum("nbk,bkj->nbj", blocked, diag_blocks, precision=PRECISE)
    positions = jnp.arange(block_count, dtype=jnp.int32)[:, None] - offsets + REACH
    products = jnp.einsum("nbk,bskj->nbsj", blocked, coupling, precision=PRECISE)
    lower_part = from_behind(vectors[:, (block_count - REACH) * block_width :], "row", 1)
    extent = block_count + REACH
    extended = jnp.concatenate([lower_part, vectors], axis=1).reshape(rowcount, extent, block_width)
    selector = one_hot_table(positions, extent)
    gathered = jnp.einsum("bse,nek->nbsk", selector, extended, precision=PRECISE)
    result = result + jnp.einsum("nbsk,bsjk->nbj", gathered, coupling, precision=PRECISE)
    spread = jnp.einsum("bse,nbsj->nej", selector, products, precision=PRECISE)
    returned = from_behind(spread[:, :REACH].reshape(rowcount, REACH * block_width), "row", -1)
    result = result + spread[:, REACH:]
    result = result.at[:, block_count - REACH :].add(returned.reshape(rowcount, REACH, block_width))
    return result.reshape(rowcount, block_count * block_width)


def padded(parts):
    count = sum(part.shape[0] for part in parts)
    return jnp.concatenate([*parts, jnp.zeros((LANES - count, parts[0].shape[1]), jnp.float32)], axis=0)


def local(diag_blocks, coupling, offsets, mass, initial_modes):
    stiff_diag = jnp.diagonal(diag_blocks, axis1=1, axis2=2).reshape(-1)
    mass_row = mass[None, :]
    stiff_initial = stiffness_apply(initial_modes, diag_blocks, coupling, offsets)
    basis, stiff_basis = padded([initial_modes]), padded([stiff_initial])
    coefficients, projected = ritz_basis(gram_pair(basis, stiff_basis, mass_row, MODES), MODES)
    modes_now = jnp.dot(coefficients, basis, precision=PRECISE)
    stiff_modes = jnp.dot(coefficients, stiff_basis, precision=PRECISE)
    directions = None
    stiff_directions = None
    for iteration in range(ITERS):
        residual = stiff_modes - jnp.dot(projected, modes_now * mass_row, precision=PRECISE)
        precond = residual / stiff_diag[None, :]
        stiff_precond = stiffness_apply(precond, diag_blocks, coupling, offsets)
        if directions is None:
            order = 2 * MODES
            basis = padded([modes_now, precond])
            stiff_basis = padded([stiff_modes, stiff_precond])
        else:
            order = 3 * MODES
            basis = padded([modes_now, precond, directions])
            stiff_basis = padded([stiff_modes, stiff_precond, stiff_directions])
        coefficients, projected = ritz_basis(gram_pair(basis, stiff_basis, mass_row, order), order)
        directions = jnp.dot(coefficients[:, MODES:], basis[MODES:], precision=PRECISE)
        stiff_directions = jnp.dot(coefficients[:, MODES:], stiff_basis[MODES:], precision=PRECISE)
        modes_now = jnp.dot(coefficients, basis, precision=PRECISE)
        stiff_modes = jnp.dot(coefficients, stiff_basis, precision=PRECISE)
    weight = mass.shape[0] * lax.axis_size("row") / MODES
    mass_density = weight * mass * jnp.sum(modes_now * modes_now, axis=0)
    energy_density = weight * jnp.sum(modes_now * stiff_modes, axis=0)
    return (mass_density, energy_density)


def solution(mesh):
    placed = (
        P(("sub", "row"), None, None),
        P(("sub", "row"), None, None, None),
        P(("sub", "row"), None),
        P(("sub", "row")),
        P(None, ("sub", "row")),
    )
    return jax.shard_map(
        local,
        mesh=mesh,
        in_specs=placed,
        out_specs=(P(("sub", "row")), P(("sub", "row"))),
        check_vma=False,
    )
```

```python
import functools

import jax
import jax.numpy as jnp
from jax import lax
from jax.experimental import pallas as pl
from jax.experimental.pallas import tpu as pltpu
from jax.sharding import PartitionSpec as P

MODES = 32
REACH = 4
ITERS = 3
PURIFY = 28
LANES = 128
TILE = 8
CHUNK = 512


PRECISE = lax.Precision.HIGHEST
MESH = pl.DeviceIdType.MESH
NT = (((1,), (1,)), ((), ()))
NN = (((1,), (0,)), ((), ()))


def dot(a, b, dims=NN):
    return lax.dot_general(a, b, dims, precision=PRECISE, preferred_element_type=jnp.float32)


def split(a):
    high = a.astype(jnp.bfloat16)
    return high, (a - high.astype(jnp.float32)).astype(jnp.bfloat16)


def dot3(a, b, dims=NN):
    (ah, al), (bh, bl) = a, b
    term = functools.partial(lax.dot_general, dimension_numbers=dims, preferred_element_type=jnp.float32)
    return term(ah, bh) + (term(ah, bl) + term(al, bh))


def copy_to(src, dst, send, recv, peer):
    return pltpu.make_async_remote_copy(
        src_ref=src, dst_ref=dst, send_sem=send, recv_sem=recv,
        device_id={"row": peer}, device_id_type=MESH)


def step_kernel(ring, order, *refs):
    count = 6 if order == MODES else 9
    inputs, refs = refs[:count], refs[count:]
    diag_ref, coup_ref, hot_ref, m_ref = inputs[:4]
    s_ref, ks_ref, out_ref = refs[:3]
    vext, aext, halo, back = refs[3:7]
    part, recv, done, send1, recv1, send2, recv2, side_send, side_recv = refs[7:]
    tiles = order // TILE
    blocks, width = diag_ref.shape[0], diag_ref.shape[1]
    length = m_ref.shape[1]
    me = lax.axis_index("row")
    barrier = pltpu.get_barrier_semaphore()

    @pl.loop(1, ring)
    def _(step):
        peer = lax.rem(me + step, ring)
        pl.semaphore_signal(barrier, inc=1, device_id={"row": peer}, device_id_type=MESH)

    if order == MODES:
        fresh = 0
        s_ref[:MODES] = inputs[4][...]
        s_ref[MODES:] = jnp.zeros((LANES - MODES, length), jnp.float32)
        ks_ref[...] = jnp.zeros((LANES, length), jnp.float32)
    else:
        fresh = MODES
        coef, h = inputs[5][...], inputs[6][...]
        if order == 3 * MODES:
            lane = lax.broadcasted_iota(jnp.int32, coef.shape, 1)
            coef = jnp.concatenate([coef, jnp.where(lane >= MODES, coef, 0.0)], axis=0)
        chunk = CHUNK if length % CHUNK == 0 else width
        for at in range(0, length, chunk):
            cut = slice(at, at + chunk)
            now = dot(coef, inputs[7][:, cut])
            stiff_now = dot(coef, inputs[8][:, cut])
            residual = stiff_now[:MODES] - dot(h, now[:MODES] * m_ref[:, cut])
            s_ref[:MODES, cut] = now[:MODES]
            ks_ref[:MODES, cut] = stiff_now[:MODES]
            s_ref[MODES : 2 * MODES, cut] = residual / inputs[4][:, cut]
            rest = LANES - 2 * MODES
            if order == 3 * MODES:
                s_ref[2 * MODES : order, cut] = now[MODES:]
                ks_ref[2 * MODES : order, cut] = stiff_now[MODES:]
                rest = LANES - order
            s_ref[LANES - rest :, cut] = jnp.zeros((rest, chunk), jnp.float32)
            ks_ref[LANES - rest :, cut] = jnp.zeros((rest, chunk), jnp.float32)

    for b in range(blocks):
        vext[b + REACH] = s_ref[fresh : fresh + MODES, b * width : (b + 1) * width]
    pl.semaphore_wait(barrier, ring - 1)
    tail = vext.at[pl.ds(blocks, REACH)]
    head = aext.at[pl.ds(0, REACH)]
    forward, backward = lax.rem(me + 1, ring), lax.rem(me + ring - 1, ring)

    def to_next():
        return copy_to(tail, halo, side_send.at[0], side_recv.at[0], forward)

    def to_previous():
        return copy_to(head, back, side_send.at[1], side_recv.at[1], backward)

    @pl.when(me < ring - 1)
    def _():
        to_next().start()

    for e in range(REACH):
        aext[e] = jnp.zeros((MODES, width), jnp.float32)
    for b in range(blocks):
        aext[b + REACH] = jnp.zeros((MODES, width), jnp.float32)

    slots = coup_ref.shape[1]

    def products(b):
        vector = split(vext[b + REACH])
        aext[b + REACH] = aext[b + REACH] + dot3(vector, split(diag_ref[b]))
        hot = hot_ref[b]
        found = [dot3(vector, split(coup_ref[b, s])) for s in range(slots)]
        for d in range(1, REACH + 1):
            total = aext[b + REACH - d]
            for s in range(slots):
                row = s * REACH + d - 1
                total = total + hot[row : row + 1] * found[s]
            aext[b + REACH - d] = total

    def gathers(b):
        hot = hot_ref[b]
        total = aext[b + REACH]
        for s in range(slots):
            seen = jnp.zeros((MODES, width), jnp.float32)
            for d in range(1, REACH + 1):
                row = s * REACH + d - 1
                seen = seen + hot[row : row + 1] * vext[b + REACH - d]
            total = total + dot3(split(seen), split(coup_ref[b, s]), NT)
        aext[b + REACH] = total

    for b in range(REACH):
        products(b)

    @pl.when(me > 0)
    def _():
        to_previous().start()

    @pl.loop(1, blocks // REACH)
    def _(group):
        for b in range(REACH):
            products(group * REACH + b)

    @pl.loop(1, blocks // REACH)
    def _(group):
        for b in range(REACH):
            gathers(group * REACH + b)

    for e in range(REACH):
        vext[e] = jnp.zeros((MODES, width), jnp.float32)

    @pl.when(me > 0)
    def _():
        to_next().wait_recv()
        vext[0:REACH] = halo[...]

    for b in range(REACH):
        gathers(b)

    @pl.when(me < ring - 1)
    def _():
        to_previous().wait_recv()
        aext[blocks : blocks + REACH] = aext[blocks : blocks + REACH] + back[...]
        to_next().wait_send()

    for b in range(blocks):
        ks_ref[fresh : fresh + MODES, b * width : (b + 1) * width] = aext[b + REACH]

    basis = s_ref[...]
    stiff = dot(basis[:order], ks_ref[...], NT)
    massed = dot(basis[:order] * m_ref[...], basis, NT)
    r = lax.broadcasted_iota(jnp.int32, (order, LANES), 0)
    c = lax.broadcasted_iota(jnp.int32, (order, LANES), 1)
    diagonal = jnp.sum(jnp.where(r == c, massed, 0.0), axis=1, keepdims=True)
    packed = jnp.where(c < order, jnp.where(r <= c, stiff, massed), jnp.where(c == order, diagonal, 0.0))
    for t in range(tiles):
        part[t] = packed[t * TILE : (t + 1) * TILE]

    def scatter(t):
        return pltpu.make_async_remote_copy(
            src_ref=part.at[t], dst_ref=recv.at[me], send_sem=send1.at[t], recv_sem=recv1.at[me],
            device_id={"row": t}, device_id_type=MESH)

    def arrival(source):
        return pltpu.make_async_remote_copy(
            src_ref=part.at[0], dst_ref=recv.at[source], send_sem=send1.at[0], recv_sem=recv1.at[source],
            device_id={"row": source}, device_id_type=MESH)

    def spread(peer):
        return pltpu.make_async_remote_copy(
            src_ref=done.at[me], dst_ref=done.at[me], send_sem=send2.at[peer], recv_sem=recv2.at[me],
            device_id={"row": peer}, device_id_type=MESH)

    def gathered(t):
        return pltpu.make_async_remote_copy(
            src_ref=done.at[t], dst_ref=done.at[t], send_sem=send2.at[0], recv_sem=recv2.at[t],
            device_id={"row": t}, device_id_type=MESH)

    @pl.loop(0, tiles)
    def _(t):
        @pl.when(t != me)
        def _():
            scatter(t).start()

    @pl.when(me < tiles)
    def _():
        recv[me] = part[me]

        @pl.loop(0, ring)
        def _(source):
            @pl.when(source != me)
            def _():
                arrival(source).wait_recv()

        done[me] = jnp.sum(recv[...], axis=0)

        @pl.loop(1, ring)
        def _(step):
            spread(lax.rem(me + step, ring)).start()

    @pl.loop(0, tiles)
    def _(t):
        @pl.when(t != me)
        def _():
            gathered(t).wait_recv()

    for t in range(tiles):
        out_ref[t * TILE : (t + 1) * TILE] = done[t]

    @pl.loop(0, tiles)
    def _(t):
        @pl.when(t != me)
        def _():
            scatter(t).wait_send()

    @pl.when(me < tiles)
    def _():
        @pl.loop(1, ring)
        def _(step):
            spread(lax.rem(me + step, ring)).wait_send()

    @pl.when(me > 0)
    def _():
        to_previous().wait_send()


def advance(order, operands, hot, mass_row, *state):
    diag_blocks, coupling = operands
    ring = lax.axis_size("row")
    tiles = order // TILE
    blocks, width = diag_blocks.shape[0], diag_blocks.shape[1]
    assert tiles <= ring and blocks % REACH == 0 and blocks >= 2 * REACH and width == LANES
    length = mass_row.shape[1]
    vmem = pl.BlockSpec(memory_space=pltpu.VMEM)
    return pl.pallas_call(
        functools.partial(step_kernel, ring, order),
        out_shape=(
            jax.ShapeDtypeStruct((LANES, length), jnp.float32),
            jax.ShapeDtypeStruct((LANES, length), jnp.float32),
            jax.ShapeDtypeStruct((order, LANES), jnp.float32),
        ),
        in_specs=[vmem] * (4 + len(state)),
        out_specs=(vmem, vmem, vmem),
        scratch_shapes=[
            pltpu.VMEM((blocks + REACH, MODES, width), jnp.float32),
            pltpu.VMEM((blocks + REACH, MODES, width), jnp.float32),
            pltpu.VMEM((REACH, MODES, width), jnp.float32),
            pltpu.VMEM((REACH, MODES, width), jnp.float32),
            pltpu.VMEM((tiles, TILE, LANES), jnp.float32),
            pltpu.VMEM((ring, TILE, LANES), jnp.float32),
            pltpu.VMEM((tiles, TILE, LANES), jnp.float32),
            pltpu.SemaphoreType.DMA((tiles,)),
            pltpu.SemaphoreType.DMA((ring,)),
            pltpu.SemaphoreType.DMA((ring,)),
            pltpu.SemaphoreType.DMA((tiles,)),
            pltpu.SemaphoreType.DMA((2,)),
            pltpu.SemaphoreType.DMA((2,)),
        ],
        compiler_params=pltpu.CompilerParams(
            collective_id=order // MODES, has_side_effects=True, vmem_limit_bytes=50 << 20),
        name=f"step{order}",
    )(diag_blocks, coupling, hot, mass_row, *state)


def eliminate(rows, other, start):
    r = lax.broadcasted_iota(jnp.int32, (MODES, 1), 0)
    scale = jnp.zeros((MODES, 1), jnp.float32)
    for j in range(MODES):
        column = rows[:, start + j : start + j + 1]
        pivot = rows[j : j + 1, start + j : start + j + 1]
        factor = jnp.where(r > j, column * (1.0 / pivot), 0.0)
        scale = jnp.where(r == j, lax.rsqrt(pivot), scale)
        top, top_other = rows[j : j + 1], other[j : j + 1]
        rows = rows - factor * top
        other = other - factor * top_other
    return rows * scale, other * scale


def ritz_kernel(order, steps_count, m_ref, coef_ref, h_ref):
    shape = (LANES, LANES)
    r = lax.broadcasted_iota(jnp.int32, shape, 0)
    c = lax.broadcasted_iota(jnp.int32, shape, 1)
    eye = (r == c) & (r < order)
    identity = jnp.where(eye, 1.0, 0.0)
    inside = (r < order) & (c < order)
    packed = m_ref[...]
    if order < LANES:
        packed = jnp.concatenate([packed, jnp.zeros((LANES - order, LANES), jnp.float32)], axis=0)
    flipped = packed.T
    g_col = lax.rsqrt(packed[:, order : order + 1] + 1e-06)
    g_row = lax.rsqrt(flipped[order : order + 1, :] + 1e-06)
    stiff = jnp.where(inside, jnp.where(r <= c, packed, flipped), 0.0)
    massed = jnp.where(inside, jnp.where(r > c, packed, flipped), 0.0)
    massed = jnp.where(eye, packed[:, order : order + 1], massed)
    stiff = g_col * stiff * g_row
    massed = g_col * massed * g_row
    bands = []
    below = identity
    for start in range(0, order, MODES):
        rows, other = eliminate(massed[start : start + MODES], below[start : start + MODES], start)
        bands.append(other)
        if start + MODES < order:
            across = rows.T
            massed = jnp.where(r >= start + MODES, massed - dot(across, rows), massed)
            below = jnp.where(r >= start + MODES, below - dot(across, other), below)
    if order < LANES:
        bands.append(jnp.zeros((LANES - order, LANES), jnp.float32))
    inverse = jnp.concatenate(bands, axis=0)
    reduced = dot(dot(inverse, stiff), inverse, NT)
    reduced = 0.5 * (reduced + reduced.T)
    if order > MODES:
        diagonal = jnp.sum(jnp.where(eye, reduced, 0.0), axis=1, keepdims=True)
        real = lax.broadcasted_iota(jnp.int32, (LANES, 1), 0) < order
        center = jnp.sum(diagonal, axis=(0, 1), keepdims=True) / order
        radius = jnp.sum(jnp.abs(reduced), axis=1, keepdims=True) - jnp.abs(diagonal)
        highest = jnp.max(jnp.where(real, diagonal + radius, -jnp.inf), axis=(0, 1), keepdims=True)
        lowest = jnp.min(jnp.where(real, diagonal - radius, jnp.inf), axis=(0, 1), keepdims=True)
        factor = jnp.minimum(
            MODES / jnp.maximum(highest - center, 1e-06),
            (order - MODES) / jnp.maximum(center - lowest, 1e-06),
        )
        initial = factor / order * (center * identity - reduced) + MODES / order * identity

        def purify_step(index, density):
            halves = split(density)
            square = dot3(halves, halves)
            cube = dot3(split(square), halves)
            numerator = jnp.sum(square * (identity - density), axis=(0, 1), keepdims=True)
            denominator = jnp.sum(jnp.where(eye, density - square, 0.0), axis=(0, 1), keepdims=True)
            safe = jnp.where(jnp.abs(denominator) > 1e-12, denominator, 1.0)
            ratio = jnp.clip(numerator / safe, 0.0, 1.0)
            up = ratio >= 0.5
            share = 1.0 / jnp.where(up, ratio, 1.0 - ratio)
            keep = jnp.where(up, 0.0, (1.0 - 2.0 * ratio) * share)
            return keep * density + share * ((1.0 + ratio) * square - cube)

        projector = lax.fori_loop(0, steps_count, purify_step, initial)
        columns = projector.T[:MODES]
        correlation = dot(columns, columns, NT)
        _, orthonormal = eliminate(correlation, columns, 0)
    else:
        orthonormal = identity[:MODES]
    coef_ref[...] = dot(orthonormal, inverse) * g_row
    half = dot(orthonormal, reduced)
    h_ref[...] = 0.5 * (dot(half, orthonormal, NT) + dot(orthonormal, half, NT))


def ritz_basis(packed, order):
    vmem = pl.BlockSpec(memory_space=pltpu.VMEM)
    return pl.pallas_call(
        functools.partial(ritz_kernel, order, PURIFY),
        out_shape=(
            jax.ShapeDtypeStruct((MODES, LANES), jnp.float32),
            jax.ShapeDtypeStruct((MODES, MODES), jnp.float32),
        ),
        in_specs=[vmem],
        out_specs=(vmem, vmem),
        name=f"ritz{order}",
    )(packed)


def one_hot_table(positions, extent):
    return (positions[..., None] == jnp.arange(extent, dtype=jnp.int32)).astype(jnp.float32)


def local(diag_blocks, coupling, offsets, mass, initial_modes):
    width = diag_blocks.shape[1]
    here = jnp.eye(width, dtype=jnp.float32)
    stiff_diag = jnp.sum(diag_blocks * here, axis=1).reshape(1, -1)
    mass_row = mass[None, :]
    operands = (diag_blocks, coupling)
    hot = one_hot_table(offsets - 1, REACH).reshape(offsets.shape[0], -1, 1)
    hot = jnp.broadcast_to(hot, (*hot.shape[:2], LANES))
    unused = jnp.zeros((1, LANES), jnp.float32)
    basis, stiff_basis, packed = advance(MODES, operands, hot, mass_row, initial_modes, unused)
    coefficients, projected = ritz_basis(packed, MODES)
    for iteration in range(ITERS):
        order = 2 * MODES if iteration == 0 else 3 * MODES
        basis, stiff_basis, packed = advance(
            order, operands, hot, mass_row, stiff_diag, coefficients, projected, basis, stiff_basis)
        coefficients, projected = ritz_basis(packed, order)
    modes_now = jnp.dot(coefficients, basis, precision=PRECISE)
    stiff_modes = jnp.dot(coefficients, stiff_basis, precision=PRECISE)
    weight = mass.shape[0] * lax.axis_size("row") / MODES
    mass_density = weight * mass * jnp.sum(modes_now * modes_now, axis=0)
    energy_density = weight * jnp.sum(modes_now * stiff_modes, axis=0)
    return (mass_density, energy_density)


def solution(mesh):
    placed = (
        P(("sub", "row"), None, None),
        P(("sub", "row"), None, None, None),
        P(("sub", "row"), None),
        P(("sub", "row")),
        P(None, ("sub", "row")),
    )
    return jax.shard_map(
        local,
        mesh=mesh,
        in_specs=placed,
        out_specs=(P(("sub", "row")), P(("sub", "row"))),
        check_vma=False,
    )
```
